128 devices in a mesh: group: 16 (over x, z), shard: 8 (over y, core).
Axes of the slice: x: 4, y: 4, z: 4, core: 2. Of those that a mesh axis runs over, the one named last changes fastest.
Arguments:
- tokens: bfloat16 [16384, 4096], P(('group', 'shard')), may hold values from -12 to 12
- out_grad: bfloat16 [16384, 4096], P(('group', 'shard')), may hold values from -12 to 12
- expert_ids: int32 [16384, 2], P(('group', 'shard')), may hold values from 0 to 7, as said below
- route_weights: bfloat16 [16384, 2], P(('group', 'shard')), may hold values from 0.099609375 to 1
- w_gate: bfloat16 [4096, 7168], P(None, 'shard'), may hold values from -0.09375 to 0.09375
- w_up: bfloat16 [4096, 7168], P(None, 'shard'), may hold values from -0.09375 to 0.09375
- w_down: bfloat16 [7168, 4096], P('shard'), may hold values from -0.0625 to 0.0625
Outputs:
- token_grad: bfloat16 [16384, 4096], P(('group', 'shard'))
- route_grad: float32 [16384, 2], P(('group', 'shard'))
- grad_gate: bfloat16 [4096, 7168], P('group', 'shard')
- grad_up: bfloat16 [4096, 7168], P('group', 'shard')
- grad_down: bfloat16 [7168, 4096], P('shard', 'group')
- grad_rms: float32 [], replicated
The draws below stay inside these ranges and needn't reach their ends.
Inputs may be any that keep to these rules, and one draw needn't show every extreme that they name: `expert_ids`: each row names two different experts. Of the 128 rows of one device, at least 12 and at most 48 name expert 0; in every draw all devices of one index of group have exactly 48 such rows.
All inputs are finite; a program needn't handle non-finite values.
Results may differ from the reference program's by a relative error of at most 0.017.
Values may be sent and summed in bfloat16 or wider, within the bound.
No kernel may reach another device: no remote copies, remote signals or barrier semaphores. Data moves between devices by JAX's collectives and lax.ppermute only.
A program may use at most 192 MiB of HBM per device.

```python
import math
import jax
import jax.numpy as jnp
from jax import lax

D = 4096
FF = 7168
EXPERTS = 8
TOK_DEV = 128
CAP = 48
TOKENS = 16384
N_GROUP = 16
N_SHARD = 8


def column_field(key, row_total, column_total):
    key_jitter, key_base = jax.random.split(key, 2)
    column_ramp = 3.0 ** (jnp.arange(column_total, dtype=jnp.float32) / column_total)
    jitter = jnp.exp(jax.random.uniform(key_jitter, (column_total,), jnp.float32, 0.0, 1.2))
    values = jax.random.normal(key_base, (row_total, column_total), jnp.float32)
    values = jnp.clip(values, -6.0, 6.0)
    return jnp.clip(0.5 * values * column_ramp * jitter, -12.0, 12.0)


def draw_tokens(key, part):
    return column_field(jax.random.fold_in(key, 11), TOKENS, D).astype(jnp.bfloat16)


def draw_out_grad(key, part):
    return column_field(jax.random.fold_in(key, 17), TOKENS, D).astype(jnp.bfloat16)


def block_ranks(block_key):
    return jax.random.permutation(block_key, TOK_DEV)


def draw_expert_ids(key, part):
    blocks = TOKENS // TOK_DEV
    key_counts, key_full, key_ranks, key_first, key_offset, key_flip = jax.random.split(jax.random.fold_in(key, 23), 6)
    counts = jax.random.randint(key_counts, (blocks,), max(CAP // 4, 1), CAP + 1)
    full_group = jax.random.randint(key_full, (), 0, blocks // N_SHARD)
    counts = jnp.where(jnp.arange(blocks) // N_SHARD == full_group, CAP, counts)
    row_ranks = jax.vmap(block_ranks)(jax.random.split(key_ranks, blocks))
    routed = (row_ranks < counts[:, None]).reshape(TOKENS)
    first_pick = jax.random.randint(key_first, (TOKENS,), 1, EXPERTS)
    offset_pick = jax.random.randint(key_offset, (TOKENS,), 1, EXPERTS - 1)
    second = 1 + (first_pick - 1 + offset_pick) % (EXPERTS - 1)
    lead_pick = jnp.where(routed, 0, second)
    flipped = jax.random.randint(key_flip, (TOKENS,), 0, 2) == 1
    left_pick = jnp.where(flipped, first_pick, lead_pick)
    right_pick = jnp.where(flipped, lead_pick, first_pick)
    return jnp.stack([left_pick, right_pick], axis=1).astype(jnp.int32)


def level_of(key, dims, cuts, least, largest):
    level, own = 1.0, jax.random.fold_in(key, 6)
    for axis_at, blocks in cuts:
        steps = jnp.exp(jax.random.uniform(jax.random.fold_in(own, axis_at), (blocks,), jnp.float32, least / len(cuts), largest / len(cuts)))
        level = level * jnp.repeat(steps, dims[axis_at] // blocks).reshape([-1 if axis == axis_at else 1 for axis in range(len(dims))])
    return level


def gaussian(key, extent, spread, bound, shards=(), kind=jnp.bfloat16):
    level = level_of(key, extent, shards, -0.22, 0.18) if shards else 1.0
    entries = jax.random.normal(key, extent, jnp.float32) * spread * level
    return jnp.minimum(jnp.maximum(entries, -bound), bound).astype(kind)


def setup_inputs(seed: int = 0) -> dict:
    splits = jax.random.split(jax.random.key(seed), 8)
    tokens = draw_tokens(jax.random.fold_in(splits[7], 71), 0)
    out_grad = draw_out_grad(jax.random.fold_in(splits[7], 71), 0)
    expert_ids = draw_expert_ids(jax.random.fold_in(splits[7], 71), 0)
    route_weights = jnp.clip(jnp.exp(math.log(1.0) - 2.306499 * jax.random.uniform(splits[3], (TOKENS, 2), jnp.float32) ** level_of(splits[3], (TOKENS, 2), ((0, 128),), -0.2, 0.2)), 0.099609375, 1.0).astype(jnp.bfloat16)
    w_gate = gaussian(splits[4], (D, FF), D ** -0.5, 0.09375, ((1, 8),))
    w_up = gaussian(splits[5], (D, FF), D ** -0.5, 0.09375, ((1, 8),))
    w_down = gaussian(splits[6], (FF, D), FF ** -0.5, 0.0625, ((0, 8),))
    return dict(tokens=tokens, out_grad=out_grad, expert_ids=expert_ids, route_weights=route_weights, w_gate=w_gate, w_up=w_up, w_down=w_down)


def pack_block(ids_block, weights_block):
    expert_hits = ids_block == 0
    routed = jnp.any(expert_hits, axis=1)
    weight = lax.optimization_barrier(jnp.sum(jnp.where(expert_hits, weights_block.astype(jnp.float32), jnp.float32(0.0)), axis=1))
    slot_order = jnp.cumsum(routed.astype(jnp.int32)) - 1
    slot_index = lax.broadcasted_iota(jnp.int32, (CAP, ids_block.shape[0]), 0)
    placing = jnp.logical_and(slot_order[None, :] == slot_index, routed[None, :]).astype(jnp.float32)
    return (expert_hits, placing, weight)

def rounded(value):
    return lax.optimization_barrier(value.astype(jnp.bfloat16)).astype(jnp.float32)

def reference(tokens, out_grad, expert_ids, route_weights, w_gate, w_up, w_down):
    row_total = N_SHARD * CAP
    tokens_grouped = tokens.reshape(N_GROUP, N_SHARD, TOK_DEV, D)
    grads_grouped = out_grad.reshape(N_GROUP, N_SHARD, TOK_DEV, D)
    ids_grouped = expert_ids.reshape(N_GROUP, N_SHARD, TOK_DEV, 2)
    weights_grouped = route_weights.reshape(N_GROUP, N_SHARD, TOK_DEV, 2)

    def one_group(totals, group_data):
        group_x, group_dy, group_ids, group_weights = group_data
        expert_hits, placing, weight = jax.vmap(pack_block)(group_ids, group_weights)
        rows_x = jnp.einsum('sct,std->scd', placing, group_x.astype(jnp.float32)).astype(jnp.bfloat16).reshape(row_total, D)
        rows_dy = jnp.einsum('sct,std->scd', placing, group_dy.astype(jnp.float32)).astype(jnp.bfloat16).reshape(row_total, D)
        rows_route = lax.optimization_barrier(jnp.sum(placing * weight[:, None, :], axis=2)).reshape(row_total, 1)
        gate_pre = jnp.dot(rows_x, w_gate, preferred_element_type=jnp.float32)
        up_pre = jnp.dot(rows_x, w_up, preferred_element_type=jnp.float32)
        hidden_grad = jnp.dot(rows_dy, w_down.T, preferred_element_type=jnp.float32)
        sigmoid_gate = jax.nn.sigmoid(gate_pre)
        activated = gate_pre * sigmoid_gate
        hidden = activated * up_pre
        route_part = lax.optimization_barrier(jnp.sum(hidden * hidden_grad, axis=1))
        weighted_hidden = (rows_route * hidden).astype(jnp.bfloat16)
        gate_grad = (rows_route * hidden_grad * up_pre * sigmoid_gate * (1.0 + gate_pre * (1.0 - sigmoid_gate))).astype(jnp.bfloat16)
        up_grad = (rows_route * hidden_grad * activated).astype(jnp.bfloat16)
        row_grads = (jnp.dot(gate_grad, w_gate.T, preferred_element_type=jnp.float32) + jnp.dot(up_grad, w_up.T, preferred_element_type=jnp.float32)).astype(jnp.bfloat16)
        token_block = jnp.einsum('sct,scd->std', placing, row_grads.reshape(N_SHARD, CAP, D).astype(jnp.float32)).astype(jnp.bfloat16)
        route_tok = jnp.einsum('sct,sc->st', placing, route_part.reshape(N_SHARD, CAP))
        route_block = jnp.where(expert_hits, route_tok[:, :, None], jnp.float32(0.0))
        part_gate = rounded(jnp.dot(rows_x.T, gate_grad, preferred_element_type=jnp.float32))
        part_up = rounded(jnp.dot(rows_x.T, up_grad, preferred_element_type=jnp.float32))
        part_down = rounded(jnp.dot(weighted_hidden.T, rows_dy, preferred_element_type=jnp.float32))
        return ((totals[0] + part_gate, totals[1] + part_up, totals[2] + part_down), (token_block, route_block))
    start_totals = (jnp.zeros((D, FF), jnp.float32), jnp.zeros((D, FF), jnp.float32), jnp.zeros((FF, D), jnp.float32))
    sums, blocks = lax.scan(one_group, start_totals, (tokens_grouped, grads_grouped, ids_grouped, weights_grouped))
    sum_gate, sum_up, sum_down = sums
    token_grad = blocks[0].reshape(N_GROUP * N_SHARD * TOK_DEV, D)
    route_grad = blocks[1].reshape(N_GROUP * N_SHARD * TOK_DEV, 2)
    square_total = jnp.sum(sum_gate * sum_gate) + jnp.sum(sum_up * sum_up) + jnp.sum(sum_down * sum_down)
    mean_sq = square_total / (3.0 * D * FF)
    inverse_rms = lax.rsqrt(mean_sq + 1e-06)
    return (token_grad, route_grad, (sum_gate * inverse_rms).astype(jnp.bfloat16), (sum_up * inverse_rms).astype(jnp.bfloat16), (sum_down * inverse_rms).astype(jnp.bfloat16), jnp.sqrt(mean_sq))
```

```python
import functools

import jax
import jax.numpy as jnp
from jax import lax
from jax.experimental import pallas as pl
from jax.experimental.pallas import tpu as pltpu
from jax.sharding import Mesh
from jax.sharding import PartitionSpec as P

D = 4096
FF = 7168
CAP = 48
TOK = 128
F = 896
DW = D + 128
ROWS = 8 * CAP
BF = jnp.bfloat16
F32 = jnp.float32
SHARD = ("y", "c")
GROUP = ("gx", "gz")
ALL = ("gx", "gz", "y", "c")


def params(**kw):
    return pltpu.CompilerParams(vmem_limit_bytes=56 * 1024 * 1024, **kw)


def shift(value, axis, step, size=4):
    return lax.ppermute(value, axis, [(i, (i + step) % size) for i in range(size)])


def dot(a, b, ca, cb):
    return lax.dot_general(a, b, (((ca,), (cb,)), ((), ())), preferred_element_type=F32)


def pack_kernel(pos, placing, tok, grad, route, packed, peer):
    gx, gz = pos[0], pos[1]
    for plane, src in enumerate((tok, grad)):
        packed[plane, :, :D] = dot(placing[...], src[...], 1, 0).astype(BF)
        packed[plane, :, D:] = route[...]
    for k in range(1, 4):
        for j in range(4):
            col = lax.rem(gx + j, 4) * 1024 + lax.rem(gz + k, 4) * 256
            for plane in range(2):
                peer[k - 1, plane, :, j * 256 : (j + 1) * 256] = packed[
                    plane, :, pl.ds(pl.multiple_of(col, 256), 256)
                ]


def pack(pos, placing, tok, grad, route):
    vmem = pl.BlockSpec(memory_space=pltpu.VMEM)
    return pl.pallas_call(
        pack_kernel,
        in_specs=[pl.BlockSpec(memory_space=pltpu.SMEM)] + [vmem] * 4,
        out_specs=[vmem, vmem],
        out_shape=[
            jax.ShapeDtypeStruct((2, CAP, DW), BF),
            jax.ShapeDtypeStruct((3, 2, CAP, 1024), BF),
        ],
        compiler_params=params(),
        name="pack",
    )(pos, placing, tok, grad, route)


KT = 512


def hidden_kernel(x, dy, route, wg, wu, wd, gg, ug, wh, part, acc_g, acc_u, acc_h):
    step = pl.program_id(0)
    xv = x[...].reshape(ROWS, KT)
    dyv = dy[...].reshape(ROWS, KT)
    pg = dot(xv, wg[...], 1, 0)
    pu = dot(xv, wu[...], 1, 0)
    ph = dot(dyv, wd[...], 1, 1)

    @pl.when(step == 0)
    def _():
        acc_g[...] = pg
        acc_u[...] = pu
        acc_h[...] = ph

    @pl.when(step > 0)
    def _():
        acc_g[...] += pg
        acc_u[...] += pu
        acc_h[...] += ph

    @pl.when(step == D // KT - 1)
    def _():
        for r in range(8):
            rows = pl.ds(r * CAP, CAP)
            w = route[r, 0, :, 0:1].astype(F32)
            gate = acc_g[rows, :]
            up = acc_u[rows, :]
            hg = acc_h[rows, :]
            s = jax.nn.sigmoid(gate)
            act = gate * s
            hidden = act * up
            part[rows, :] = jnp.broadcast_to(
                jnp.sum(hidden * hg, axis=1, keepdims=True), (CAP, 128)
            )
            wh[rows, :] = (w * hidden).astype(BF)
            whg = w * hg
            gg[rows, :] = (whg * up * s * (1.0 + gate * (1.0 - s))).astype(BF)
            ug[rows, :] = (whg * act).astype(BF)


def hidden_grads(rows, wg, wu, wd):
    full = lambda shape: pl.BlockSpec(shape, lambda k: (0, 0))
    return pl.pallas_call(
        hidden_kernel,
        grid=(D // KT,),
        in_specs=[
            pl.BlockSpec((8, 1, CAP, KT), lambda k: (0, 0, 0, k)),
            pl.BlockSpec((8, 1, CAP, KT), lambda k: (0, 1, 0, k)),
            pl.BlockSpec((8, 1, CAP, 128), lambda k: (0, 0, 0, D // 128)),
            pl.BlockSpec((KT, F), lambda k: (k, 0)),
            pl.BlockSpec((KT, F), lambda k: (k, 0)),
            pl.BlockSpec((F, KT), lambda k: (0, k)),
        ],
        out_specs=[full((ROWS, F))] * 3 + [full((ROWS, 128))],
        out_shape=[jax.ShapeDtypeStruct((ROWS, F), BF)] * 3
        + [jax.ShapeDtypeStruct((ROWS, 128), F32)],
        scratch_shapes=[pltpu.VMEM((ROWS, F), F32)] * 3,
        compiler_params=params(dimension_semantics=("arbitrary",)),
        cost_estimate=pl.CostEstimate(
            flops=6 * ROWS * D * F, bytes_accessed=28 * 2**20, transcendentals=ROWS * F
        ),
        name="hidden",
    )(rows, rows, rows, wg, wu, wd)


ST = 1408


def slot_kernel(gg, ug, part, wg, wu, out):
    acc = dot(gg[...], wg[...], 1, 1) + dot(ug[...], wu[...], 1, 1)
    out[...] = acc.astype(BF).reshape(8, CAP, ST)

    @pl.when(pl.program_id(0) == DW // ST - 1)
    def _():
        high = part[...].astype(BF)
        low = (part[...] - high.astype(F32)).astype(BF)
        lane = lax.broadcasted_iota(jnp.int32, (ROWS, 128), 1)
        both = jnp.where(lane < 64, high.astype(F32), low.astype(F32)).astype(BF)
        out[:, :, ST - 128 :] = both.reshape(8, CAP, 128)


def slot_grads(gg, ug, part, wg, wu):
    full = lambda shape: pl.BlockSpec(shape, lambda k: (0, 0))
    return pl.pallas_call(
        slot_kernel,
        grid=(DW // ST,),
        in_specs=[
            full((ROWS, F)),
            full((ROWS, F)),
            full((ROWS, 128)),
            pl.BlockSpec((ST, F), lambda k: (k, 0)),
            pl.BlockSpec((ST, F), lambda k: (k, 0)),
        ],
        out_specs=pl.BlockSpec((8, CAP, ST), lambda k: (0, 0, k)),
        out_shape=jax.ShapeDtypeStruct((8, CAP, DW), BF),
        compiler_params=params(dimension_semantics=("arbitrary",)),
        cost_estimate=pl.CostEstimate(
            flops=4 * ROWS * D * F, bytes_accessed=18 * 2**20, transcendentals=0
        ),
        name="slot",
    )(gg, ug, part, wg, wu)


def block_of(order, own, peers, hidden_all, transpose, xs):
    xs[0:ROWS, :] = own[...].reshape(ROWS, 256)
    for k in range(3):
        xs[(k + 1) * ROWS : (k + 2) * ROWS, :] = peers[:, k].reshape(ROWS, 256)
    if transpose:
        return dot(hidden_all[...], xs[...], 0, 0)
    return dot(xs[...], hidden_all[...], 0, 0)


def stage_hidden(h0, h1, h2a, h2b, h3, hs):
    half = ROWS // 2
    hs[0:ROWS, :] = h0[...]
    hs[ROWS : 2 * ROWS, :] = h1[...]
    hs[2 * ROWS : 2 * ROWS + half, :] = h2a[...]
    hs[2 * ROWS + half : 3 * ROWS, :] = h2b[...]
    hs[3 * ROWS :, :] = h3[...]


def far_kernel(transpose, pos, own, peers, h0, h1, h2a, h2b, h3, top, low, hs, xs):
    stage_hidden(h0, h1, h2a, h2b, h3, hs)
    value = block_of(0, own, peers, hs, transpose, xs).astype(BF)
    n = value.shape[0] // 2
    top[...] = value[:n]
    low[...] = value[n:]


def near_kernel(
    transpose, pos, own, peers, h0, h1, h2a, h2b, h3, fa, fb, plus, minus, keep, hs, xs
):
    step = pl.program_id(0)

    @pl.when(step == 0)
    def _():
        stage_hidden(h0, h1, h2a, h2b, h3, hs)

    value = block_of(0, own, peers, hs, transpose, xs)
    n = value.shape[0] // 2

    @pl.when(step == 0)
    def _():
        plus[:n] = (value[:n] + fa[...].astype(F32)).astype(BF)
        plus[n:] = value[n:].astype(BF)

    @pl.when(step == 1)
    def _():
        minus[:n] = value[:n].astype(BF)
        minus[n:] = (value[n:] + fb[...].astype(F32)).astype(BF)

    @pl.when(step == 2)
    def _():
        keep[...] = value


def grad_specs(plane, offset):
    def own_map(i, pos):
        return (0, plane, 0, lax.rem(pos[0] + offset(i), 4) * 4 + pos[1])

    def peer_map(i, pos):
        return (0, 0, plane, 0, offset(i))

    full = pl.BlockSpec((ROWS, F), lambda i, pos: (0, 0))
    half = pl.BlockSpec((ROWS // 2, F), lambda i, pos: (0, 0))
    return [
        pl.BlockSpec((8, 1, CAP, 256), own_map),
        pl.BlockSpec((8, 3, 1, CAP, 256), peer_map),
        full,
        full,
        half,
        half,
        full,
    ]


SCRATCH = [pltpu.VMEM((4 * ROWS, F), BF), pltpu.VMEM((4 * ROWS, 256), BF)]


def far_block(pos, rows, peers, hidden, plane):
    transpose = plane == 1
    shape = (F // 2, 256) if transpose else (128, F)
    return pl.pallas_call(
        functools.partial(far_kernel, transpose),
        grid_spec=pltpu.PrefetchScalarGridSpec(
            num_scalar_prefetch=1,
            grid=(1,),
            in_specs=grad_specs(plane, lambda i: i + 2),
            out_specs=[pl.BlockSpec(shape, lambda i, pos: (0, 0))] * 2,
            scratch_shapes=SCRATCH,
        ),
        out_shape=[jax.ShapeDtypeStruct(shape, BF)] * 2,
        compiler_params=params(),
        cost_estimate=pl.CostEstimate(
            flops=2 * 4 * ROWS * 256 * F, bytes_accessed=4 * 2**20, transcendentals=0
        ),
        name="far",
    )(pos, rows, peers, *hidden)


def near_blocks(pos, rows, peers, hidden, fa, fb, plane):
    transpose = plane == 1
    shape = (F, 256) if transpose else (256, F)
    halves = pl.BlockSpec((shape[0] // 2, shape[1]), lambda i, pos: (0, 0))
    offset = lambda i: lax.rem(2 * i + 1, 4) * (1 - i // 2)
    return pl.pallas_call(
        functools.partial(near_kernel, transpose),
        grid_spec=pltpu.PrefetchScalarGridSpec(
            num_scalar_prefetch=1,
            grid=(3,),
            in_specs=grad_specs(plane, offset) + [halves, halves],
            out_specs=[pl.BlockSpec(shape, lambda i, pos: (0, 0))] * 3,
            scratch_shapes=SCRATCH,
        ),
        out_shape=[
            jax.ShapeDtypeStruct(shape, BF),
            jax.ShapeDtypeStruct(shape, BF),
            jax.ShapeDtypeStruct(shape, F32),
        ],
        compiler_params=params(dimension_semantics=("arbitrary",)),
        cost_estimate=pl.CostEstimate(
            flops=6 * 4 * ROWS * 256 * F, bytes_accessed=8 * 2**20, transcendentals=0
        ),
        name="near",
    )(pos, rows, peers, *hidden, fa, fb)


def ring_gather(value, axis):
    half = value.shape[0] // 2
    behind = shift(value, axis, 1)
    ahead = shift(value, axis, -1)
    far_a = shift(behind[:half], axis, 1)
    far_b = shift(ahead[half:], axis, -1)
    return value, behind, far_a, far_b, ahead


def pack_rows(expert_ids, route_weights):
    hits = expert_ids == 0
    routed = jnp.any(hits, axis=1)
    weight = jnp.sum(jnp.where(hits, route_weights.astype(F32), 0.0), axis=1)
    order = jnp.cumsum(routed.astype(jnp.int32)) - 1
    slot = lax.broadcasted_iota(jnp.int32, (CAP, TOK), 0)
    placing = jnp.logical_and(order[None, :] == slot, routed[None, :])
    return hits, placing, weight


def body(tokens, out_grad, expert_ids, route_weights, w_gate, w_up, w_down):
    pos = jnp.stack([lax.axis_index("gx"), lax.axis_index("gz")]).astype(jnp.int32)
    hits, placing, weight = pack_rows(expert_ids, route_weights)
    placing_bf = placing.astype(BF)
    route = jnp.sum(placing.astype(F32) * weight[None, :], axis=1, keepdims=True)
    route = jnp.broadcast_to(route, (CAP, 128)).astype(BF)
    packed, peer = pack(pos, placing_bf, tokens, out_grad, route)
    rows = lax.all_gather(packed, SHARD, axis=0, tiled=False)
    mine = jnp.stack([shift(peer[k - 1], "gz", k) for k in (1, 2, 3)])
    peers = lax.all_gather(mine, SHARD, axis=0, tiled=False)
    gg, ug, wh, part = hidden_grads(rows, w_gate, w_up, w_down)

    sums = {}
    for name, value, plane in (("down", wh, 1), ("gate", gg, 0), ("up", ug, 0)):
        hidden = ring_gather(value, "gz")
        top, low = far_block(pos, rows, peers, hidden, plane)
        fa = shift(top, "gx", 1)
        fb = shift(low, "gx", -1)
        plus, minus, keep = near_blocks(pos, rows, peers, hidden, fa, fb, plane)
        a = shift(plus, "gx", 1)
        b = shift(minus, "gx", -1)
        sums[name] = keep + a.astype(F32) + b.astype(F32)

    slots = slot_grads(gg, ug, part, w_gate, w_up)
    back = lax.psum_scatter(slots, SHARD, scatter_dimension=0, tiled=False)
    token_grad = dot(placing_bf, back[:, :D], 0, 0).astype(BF)
    back_route = back[:, D].astype(F32) + back[:, D + 64].astype(F32)
    route_tok = jnp.sum(placing.astype(F32) * back_route[:, None], axis=0)
    route_grad = jnp.where(hits, route_tok[:, None], 0.0)

    local_sq = sum(jnp.sum(v * v) for v in sums.values())
    every = lax.all_to_all(jnp.broadcast_to(local_sq, (128, 128)), ALL, 0, 0, tiled=True)
    mean_sq = jnp.sum(every[:, 0]) / (3.0 * D * FF)
    inverse = lax.rsqrt(mean_sq + 1e-06)
    return (
        token_grad,
        route_grad,
        (sums["gate"] * inverse).astype(BF),
        (sums["up"] * inverse).astype(BF),
        (sums["down"] * inverse).astype(BF),
        jnp.sqrt(mean_sq),
    )


def solution(mesh):
    split = Mesh(mesh.devices.reshape(4, 4, 4, 2), ALL)
    return jax.shard_map(
        body,
        mesh=split,
        in_specs=(
            P(ALL, None),
            P(ALL, None),
            P(ALL, None),
            P(ALL, None),
            P(None, SHARD),
            P(None, SHARD),
            P(SHARD, None),
        ),
        out_specs=(
            P(ALL, None),
            P(ALL, None),
            P(GROUP, SHARD),
            P(GROUP, SHARD),
            P(SHARD, GROUP),
            P(),
        ),
        check_vma=False,
    )
```
